32 devices in a mesh: seq: 16 (over z, y, x), rep: 2 (over core).
Axes of the slice: x: 2, y: 2, z: 4, core: 2. Of those that a mesh axis runs over, the one named last changes fastest.
Arguments:
- q_lin: bfloat16 [2, 2048, 4096], P('rep', 'seq'), may hold values from -90 to 90, as said below
- k_lin: bfloat16 [2, 2048, 512], P('rep', 'seq'), may hold values from -4 to 4
- value_projection: bfloat16 [2, 2048, 512], P('rep', 'seq'), may hold values from -6 to 6
- grad_out: bfloat16 [2, 2048, 4096], P('rep', 'seq'), may hold values from -6 to 6
- q_bias: float32 [4096], replicated, may hold values from -3 to 3
- block_lists: int32 [32, 16, 2], replicated, may hold values from 0 to 15, as said below
- block_counts: int32 [32, 16], replicated, may hold values from 1 to 2, as said below
Outputs:
- dq: bfloat16 [2, 2048, 4096], P('rep', 'seq')
- dk: bfloat16 [2, 2048, 512], P('rep', 'seq')
- dv: bfloat16 [2, 2048, 512], P('rep', 'seq')
- dbq: float32 [4096], replicated
The draws below stay inside these ranges and needn't reach their ends.
Inputs may be any that keep to these rules, and one draw needn't show every extreme that they name: `q_lin`: in the shown and hidden draws alike the entries stay within the stated range. `block_lists`: entry 0 of every list is the query block itself; the 2 entries of a list are distinct; entries past block_counts are ignored. `block_counts`: some head has 2 for every query block.
All inputs are finite; a program needn't handle non-finite values.
Results may differ from the reference program's by a relative error of at most 0.008.
Values may be sent and summed in bfloat16 or wider, within the bound.
A program may use at most 128 MiB of HBM per device.

```python
import jax
import jax.numpy as jnp
from jax import lax

QUERY_HEADS = 32
KEY_VALUE_HEADS = 4
HEAD_WIDTH = 128
BLOCK = 128
SEL = 2
SEQUENCE_LENGTH = 2048
BATCH_COUNT = 2
QBLOCKS = 16
GROUP_SIZE = 8


def query_key_pair(key):
    base = jax.random.fold_in(key, 11)
    key_query, key_random_keys = jax.random.split(base, 2)
    gathered_keys = jnp.clip(jax.random.normal(key_random_keys, (BATCH_COUNT, SEQUENCE_LENGTH, KEY_VALUE_HEADS, HEAD_WIDTH), jnp.float32), -4.0, 4.0)
    query_rows = jnp.clip(jax.random.normal(key_query, (BATCH_COUNT, SEQUENCE_LENGTH, QUERY_HEADS, HEAD_WIDTH), jnp.float32), -4.0, 4.0)
    return (query_rows.reshape(BATCH_COUNT, SEQUENCE_LENGTH, QUERY_HEADS * HEAD_WIDTH), gathered_keys.reshape(BATCH_COUNT, SEQUENCE_LENGTH, KEY_VALUE_HEADS * HEAD_WIDTH))


def draw_q_lin(key, part):
    return query_key_pair(key)[0].astype(jnp.bfloat16)


def draw_k_lin(key, part):
    return query_key_pair(key)[1].astype(jnp.bfloat16)


def mask_tables(key):
    base = jax.random.fold_in(key, 7)
    key_levels, key_heavy, key_shift, key_picks = jax.random.split(base, 4)
    levels = jax.random.randint(key_levels, (QUERY_HEADS,), 1, SEL + 1)
    heavy = jax.random.randint(key_heavy, (), 0, QUERY_HEADS)
    shifts = jax.random.randint(key_shift, (QUERY_HEADS, QBLOCKS), 0, 2)
    counts = jnp.clip(levels[:, None] - shifts, 1, SEL)
    counts = counts.at[heavy].set(SEL)
    row_keys = jax.random.split(key_picks, QUERY_HEADS * QBLOCKS)
    others = jax.vmap(lambda row_key: jax.random.permutation(row_key, QBLOCKS - 1)[:SEL - 1])(row_keys)
    others = others.reshape(QUERY_HEADS, QBLOCKS, SEL - 1)
    own = jnp.broadcast_to(jnp.arange(QBLOCKS, dtype=jnp.int32)[None, :, None], (QUERY_HEADS, QBLOCKS, 1))
    others = (own + 1 + others) % QBLOCKS
    chosen = jnp.concatenate([own, others.astype(jnp.int32)], axis=2)
    return (chosen.astype(jnp.int32), counts.astype(jnp.int32))


def draw_block_lists(key, part):
    return mask_tables(key)[0]


def draw_block_counts(key, part):
    return mask_tables(key)[1]


def block_scale(own_key, extent, shards, low, top_value):
    def one(position, parts):
        draws = jax.random.uniform(jax.random.fold_in(jax.random.fold_in(own_key, 6), position), (parts,), jnp.float32, low / len(shards), top_value / len(shards))
        return jnp.repeat(jnp.exp(draws), extent[position] // parts).reshape((-1,) + (1,) * (len(extent) - position - 1))

    factor_of = one(*shards[0])
    for cut in shards[1:]:
        factor_of = factor_of * one(*cut)
    return factor_of


def normal_values(key, dims, width, most, cuts=(), kind=jnp.bfloat16):
    gain = block_scale(key, dims, cuts, -0.22, 0.18) if cuts else 1.0
    drawn = jax.random.normal(key, dims, jnp.float32) * width * gain
    return jnp.minimum(jnp.maximum(drawn, -most), most).astype(kind)


def setup_inputs(seed: int = 0) -> dict:
    keys = jax.random.split(jax.random.key(seed), 8)
    return {
        "q_lin": draw_q_lin(jax.random.fold_in(keys[7], 71), 0),
        "k_lin": draw_k_lin(jax.random.fold_in(keys[7], 71), 0),
        "value_projection": normal_values(keys[2], (BATCH_COUNT, SEQUENCE_LENGTH, KEY_VALUE_HEADS * HEAD_WIDTH), 1.0, 6.0, ((0, 2), (1, 16))),
        "grad_out": normal_values(keys[3], (BATCH_COUNT, SEQUENCE_LENGTH, QUERY_HEADS * HEAD_WIDTH), 1.0, 6.0, ((0, 2), (1, 16))),
        "q_bias": normal_values(keys[4], (QUERY_HEADS * HEAD_WIDTH,), 0.5, 3.0, (), jnp.float32),
        "block_lists": draw_block_lists(jax.random.fold_in(keys[7], 71), 0),
        "block_counts": draw_block_counts(jax.random.fold_in(keys[7], 71), 0),
    }


def rounded(values_in):
    return lax.optimization_barrier(values_in.astype(jnp.bfloat16)).astype(jnp.float32)


def head_pass(query_rows, key_rows, value_rows, grads, chosen, counts):
    scaling = HEAD_WIDTH ** -0.5
    q_blocks = query_rows.reshape(QBLOCKS, BLOCK, HEAD_WIDTH).astype(jnp.float32)
    key_sel = key_rows.reshape(QBLOCKS, BLOCK, HEAD_WIDTH)[chosen].reshape(QBLOCKS, SEL * BLOCK, HEAD_WIDTH).astype(jnp.float32)
    value_sel = value_rows.reshape(QBLOCKS, BLOCK, HEAD_WIDTH)[chosen].reshape(QBLOCKS, SEL * BLOCK, HEAD_WIDTH).astype(jnp.float32)
    g_blocks = grads.reshape(QBLOCKS, BLOCK, HEAD_WIDTH).astype(jnp.float32)
    active = jnp.repeat(jnp.arange(SEL, dtype=jnp.int32)[None, :] < counts[:, None], BLOCK, axis=1)
    scores = jnp.einsum("qrd,qkd->qrk", q_blocks, key_sel) * scaling
    scores = jnp.where(active[:, None, :], scores, -1.0e30)
    weights = jax.nn.softmax(scores, axis=-1)
    weights_half = rounded(weights)
    attn_out = jnp.einsum("qrk,qkd->qrd", weights_half, value_sel)
    row_dots = jnp.sum(g_blocks * attn_out, axis=-1)
    weight_grads = jnp.einsum("qrd,qkd->qrk", g_blocks, value_sel)
    score_grads = rounded(weights * (weight_grads - row_dots[..., None]))
    grad_q = scaling * jnp.einsum("qrk,qkd->qrd", score_grads, key_sel)
    dk_sel = scaling * jnp.einsum("qrk,qrd->qkd", score_grads, q_blocks)
    dv_sel = jnp.einsum("qrk,qrd->qkd", weights_half, g_blocks)
    empty = jnp.zeros((QBLOCKS, BLOCK, HEAD_WIDTH), jnp.float32)
    key_gradient = empty.at[chosen].add(dk_sel.reshape(QBLOCKS, SEL, BLOCK, HEAD_WIDTH))
    value_gradient = empty.at[chosen].add(dv_sel.reshape(QBLOCKS, SEL, BLOCK, HEAD_WIDTH))
    return grad_q.reshape(SEQUENCE_LENGTH, HEAD_WIDTH), key_gradient.reshape(SEQUENCE_LENGTH, HEAD_WIDTH), value_gradient.reshape(SEQUENCE_LENGTH, HEAD_WIDTH)


def reference(q_lin, k_lin, value_projection, grad_out, q_bias, block_lists, block_counts):
    query_rows = (q_lin.astype(jnp.float32) + q_bias).astype(jnp.bfloat16)
    group_of = jnp.arange(QUERY_HEADS, dtype=jnp.int32) // GROUP_SIZE

    def per_sequence(members):
        q_seq, key_sequence, value_sequence, g_seq = members
        q_heads = jnp.transpose(q_seq.reshape(SEQUENCE_LENGTH, QUERY_HEADS, HEAD_WIDTH), (1, 0, 2))
        g_heads = jnp.transpose(g_seq.reshape(SEQUENCE_LENGTH, QUERY_HEADS, HEAD_WIDTH), (1, 0, 2))
        key_head_rows = jnp.transpose(key_sequence.reshape(SEQUENCE_LENGTH, KEY_VALUE_HEADS, HEAD_WIDTH), (1, 0, 2))
        value_head_rows = jnp.transpose(value_sequence.reshape(SEQUENCE_LENGTH, KEY_VALUE_HEADS, HEAD_WIDTH), (1, 0, 2))

        def per_head(inner):
            q_one, g_one, chosen, counts, group = inner
            key_rows = lax.dynamic_index_in_dim(key_head_rows, group, 0, keepdims=False)
            value_rows = lax.dynamic_index_in_dim(value_head_rows, group, 0, keepdims=False)
            return head_pass(q_one, key_rows, value_rows, g_one, chosen, counts)

        grad_q, key_gradient, value_gradient = lax.map(per_head, (q_heads, g_heads, block_lists, block_counts, group_of))
        bias_part = jnp.sum(grad_q, axis=1)
        dq_seq = jnp.transpose(grad_q, (1, 0, 2)).reshape(SEQUENCE_LENGTH, QUERY_HEADS * HEAD_WIDTH).astype(jnp.bfloat16)
        key_gradient_sequence = jnp.sum(key_gradient.reshape(KEY_VALUE_HEADS, GROUP_SIZE, SEQUENCE_LENGTH, HEAD_WIDTH), axis=1)
        value_gradient_sequence = jnp.sum(value_gradient.reshape(KEY_VALUE_HEADS, GROUP_SIZE, SEQUENCE_LENGTH, HEAD_WIDTH), axis=1)
        key_gradient_sequence = jnp.transpose(key_gradient_sequence, (1, 0, 2)).reshape(SEQUENCE_LENGTH, KEY_VALUE_HEADS * HEAD_WIDTH).astype(jnp.bfloat16)
        value_gradient_sequence = jnp.transpose(value_gradient_sequence, (1, 0, 2)).reshape(SEQUENCE_LENGTH, KEY_VALUE_HEADS * HEAD_WIDTH).astype(jnp.bfloat16)
        return dq_seq, key_gradient_sequence, value_gradient_sequence, bias_part

    dq, dk, dv, bias_parts = lax.map(per_sequence, (query_rows, k_lin, value_projection, grad_out))
    return dq, dk, dv, jnp.sum(bias_parts, axis=0).reshape(QUERY_HEADS * HEAD_WIDTH)
```

```python
import functools

import jax
import jax.numpy as jnp
from jax import lax
from jax.experimental import pallas as pl
from jax.experimental.pallas import tpu as pltpu
from jax.sharding import PartitionSpec as P

NT = (((1,), (1,)), ((), ()))
TN = (((0,), (0,)), ((), ()))
NN = (((1,), (0,)), ((), ()))


def dot(a, b, dims):
    return lax.dot_general(a, b, dims, preferred_element_type=jnp.float32)


def attend_kernel(
    head_dim, group, scaling,
    other_ref, count_ref,
    q_ref, g_ref, bias_ref, k_ref, v_ref, kall_ref, vall_ref,
    dq_ref, part_k_ref, part_v_ref, own_k_ref, own_v_ref, dbq_ref,
    acc_k, acc_v,
):
    step = pl.program_id(0)
    acc_k[...] = jnp.zeros_like(acc_k)
    acc_v[...] = jnp.zeros_like(acc_v)
    own_k_ref[...] = jnp.zeros_like(own_k_ref)
    own_v_ref[...] = jnp.zeros_like(own_v_ref)
    for member in range(group):
        head = step * group + member
        columns = slice(member * head_dim, (member + 1) * head_dim)
        count = count_ref[head]
        other = other_ref[head]

        def finish(queries, grad_q):
            dq_ref[:, columns] = grad_q.astype(jnp.bfloat16)
            dbq_ref[:, columns] = jnp.sum(grad_q, axis=0, keepdims=True)

        def rows():
            queries = (q_ref[:, columns].astype(jnp.float32) + bias_ref[:, columns]).astype(
                jnp.bfloat16
            )
            return queries, g_ref[:, columns]

        @pl.when(count == 1)
        def _():
            queries, grads = rows()
            keys, values = k_ref[...], v_ref[...]
            scores = dot(keys, queries, NT) * scaling
            weights = jnp.exp(scores - jnp.max(scores, axis=0, keepdims=True))
            weights = weights / jnp.sum(weights, axis=0, keepdims=True)
            half = weights.astype(jnp.bfloat16)
            weight_grads = dot(values, grads, NT)
            row_dots = jnp.sum(half.astype(jnp.float32) * weight_grads, axis=0, keepdims=True)
            score_grads = (weights * (weight_grads - row_dots)).astype(jnp.bfloat16)
            finish(queries, scaling * dot(score_grads, keys, TN))
            own_k_ref[...] += dot(score_grads, queries, NN)
            own_v_ref[...] += dot(half, grads, NN)

        @pl.when(count != 1)
        def _():
            queries, grads = rows()
            keys = [k_ref[...], kall_ref[other]]
            values = [v_ref[...], vall_ref[other]]
            scores = [dot(one, queries, NT) * scaling for one in keys]
            top = jnp.maximum(
                jnp.max(scores[0], axis=0, keepdims=True), jnp.max(scores[1], axis=0, keepdims=True)
            )
            weights = [jnp.exp(one - top) for one in scores]
            total = jnp.sum(weights[0], axis=0, keepdims=True) + jnp.sum(
                weights[1], axis=0, keepdims=True
            )
            weights = [one / total for one in weights]
            half = [one.astype(jnp.bfloat16) for one in weights]
            weight_grads = [dot(one, grads, NT) for one in values]
            row_dots = sum(
                jnp.sum(a.astype(jnp.float32) * b, axis=0, keepdims=True)
                for a, b in zip(half, weight_grads)
            )
            score_grads = [
                (a * (b - row_dots)).astype(jnp.bfloat16) for a, b in zip(weights, weight_grads)
            ]
            finish(
                queries,
                scaling * (dot(score_grads[0], keys[0], TN) + dot(score_grads[1], keys[1], TN)),
            )
            own_k_ref[...] += dot(score_grads[0], queries, NN)
            own_v_ref[...] += dot(half[0], grads, NN)
            acc_k[other] += dot(score_grads[1], queries, NN)
            acc_v[other] += dot(half[1], grads, NN)

    own_k_ref[...] = own_k_ref[...] * scaling
    part_k_ref[...] = (acc_k[...] * scaling).astype(jnp.bfloat16)
    part_v_ref[...] = acc_v[...].astype(jnp.bfloat16)


def attend(q, g, bias, k, v, kall, vall, other, count):
    rows, width = q.shape
    blocks = kall.shape[0]
    heads = other.shape[0]
    head_dim = width // heads
    kv_count = k.shape[1] // head_dim
    group = heads // kv_count
    wide = pl.BlockSpec((rows, group * head_dim), lambda s, *_: (0, s))
    thin = pl.BlockSpec((rows, head_dim), lambda s, *_: (0, s))
    line = pl.BlockSpec((1, group * head_dim), lambda s, *_: (0, s))
    whole = pl.BlockSpec((blocks, rows, head_dim), lambda s, *_: (0, 0, s))
    return pl.pallas_call(
        functools.partial(attend_kernel, head_dim, group, head_dim ** (-0.5)),
        grid_spec=pltpu.PrefetchScalarGridSpec(
            num_scalar_prefetch=2,
            grid=(kv_count,),
            in_specs=[wide, wide, line, thin, thin, whole, whole],
            out_specs=[wide, whole, whole, thin, thin, line],
            scratch_shapes=[
                pltpu.VMEM((blocks, rows, head_dim), jnp.float32),
                pltpu.VMEM((blocks, rows, head_dim), jnp.float32),
            ],
        ),
        out_shape=[
            jax.ShapeDtypeStruct((rows, width), jnp.bfloat16),
            jax.ShapeDtypeStruct(kall.shape, jnp.bfloat16),
            jax.ShapeDtypeStruct(vall.shape, jnp.bfloat16),
            jax.ShapeDtypeStruct(k.shape, jnp.float32),
            jax.ShapeDtypeStruct(v.shape, jnp.float32),
            jax.ShapeDtypeStruct((1, width), jnp.float32),
        ],
        compiler_params=pltpu.CompilerParams(vmem_limit_bytes=56 * 1024 * 1024),
        name="attend",
    )(other, count, q, g, bias, k, v, kall, vall)


def body(q_lin, k_lin, value_projection, grad_out, q_bias, block_lists, block_counts):
    me = lax.axis_index("seq")
    assert block_lists.shape[1] == lax.axis_size("seq") and block_lists.shape[2] == 2
    lists = lax.dynamic_index_in_dim(block_lists, me, 1, keepdims=False)
    count = lax.dynamic_index_in_dim(block_counts, me, 1, keepdims=False)
    other = jnp.clip(lists[:, 1], 0, block_lists.shape[1] - 1)
    kall = lax.all_gather(k_lin[0], "seq", axis=0)
    vall = lax.all_gather(value_projection[0], "seq", axis=0)
    dq, part_k, part_v, own_k, own_v, dbq = attend(
        q_lin[0], grad_out[0], q_bias[None], k_lin[0], value_projection[0], kall, vall, other, count
    )
    dbq = lax.psum(dbq[0], ("seq", "rep"))
    sum_k = lax.psum_scatter(part_k, "seq", scatter_dimension=0)
    sum_v = lax.psum_scatter(part_v, "seq", scatter_dimension=0)
    dk = (own_k + sum_k.astype(jnp.float32)).astype(jnp.bfloat16)
    dv = (own_v + sum_v.astype(jnp.float32)).astype(jnp.bfloat16)
    return (dq[None], dk[None], dv[None], dbq)


def solution(mesh):
    placed = (P("rep", "seq", None),) * 4 + (P(),) * 3
    return jax.shard_map(
        body,
        mesh=mesh,
        in_specs=placed,
        out_specs=(P("rep", "seq", None),) * 3 + (P(),),
        check_vma=False,
    )
```

```python
import functools

import jax
import jax.numpy as jnp
from jax import lax
from jax.experimental import pallas as pl
from jax.experimental.pallas import tpu as pltpu
from jax.sharding import PartitionSpec as P

NT = (((1,), (1,)), ((), ()))
TN = (((0,), (0,)), ((), ()))
NN = (((1,), (0,)), ((), ()))


def dot(a, b, dims):
    return lax.dot_general(a, b, dims, preferred_element_type=jnp.float32)


def attend_kernel(
    head_dim, group, scaling,
    other_ref, count_ref,
    q_ref, g_ref, bias_ref, k_ref, v_ref, kall_ref, vall_ref,
    dq_ref, part_k_ref, part_v_ref, own_k_ref, own_v_ref, dbq_ref,
    acc_k, acc_v,
):
    step = pl.program_id(0)
    acc_k[...] = jnp.zeros_like(acc_k)
    acc_v[...] = jnp.zeros_like(acc_v)
    own_k_ref[...] = jnp.zeros_like(own_k_ref)
    own_v_ref[...] = jnp.zeros_like(own_v_ref)
    for member in range(group):
        head = step * group + member
        columns = slice(member * head_dim, (member + 1) * head_dim)
        count = count_ref[head]
        other = other_ref[head]

        def finish(queries, grad_q):
            dq_ref[:, columns] = grad_q.astype(jnp.bfloat16)
            dbq_ref[:, columns] = jnp.sum(grad_q, axis=0, keepdims=True)

        def rows():
            queries = (q_ref[:, columns].astype(jnp.float32) + bias_ref[:, columns]).astype(
                jnp.bfloat16
            )
            return queries, g_ref[:, columns]

        @pl.when(count == 1)
        def _():
            queries, grads = rows()
            keys, values = k_ref[...], v_ref[...]
            scores = dot(keys, queries, NT) * scaling
            weights = jnp.exp(scores - jnp.max(scores, axis=0, keepdims=True))
            weights = weights / jnp.sum(weights, axis=0, keepdims=True)
            half = weights.astype(jnp.bfloat16)
            weight_grads = dot(values, grads, NT)
            row_dots = jnp.sum(half.astype(jnp.float32) * weight_grads, axis=0, keepdims=True)
            score_grads = (weights * (weight_grads - row_dots)).astype(jnp.bfloat16)
            finish(queries, scaling * dot(score_grads, keys, TN))
            own_k_ref[...] += dot(score_grads, queries, NN)
            own_v_ref[...] += dot(half, grads, NN)

        @pl.when(count != 1)
        def _():
            queries, grads = rows()
            keys = [k_ref[...], kall_ref[other]]
            values = [v_ref[...], vall_ref[other]]
            scores = [dot(one, queries, NT) * scaling for one in keys]
            top = jnp.maximum(
                jnp.max(scores[0], axis=0, keepdims=True), jnp.max(scores[1], axis=0, keepdims=True)
            )
            weights = [jnp.exp(one - top) for one in scores]
            total = jnp.sum(weights[0], axis=0, keepdims=True) + jnp.sum(
                weights[1], axis=0, keepdims=True
            )
            weights = [one / total for one in weights]
            half = [one.astype(jnp.bfloat16) for one in weights]
            weight_grads = [dot(one, grads, NT) for one in values]
            row_dots = sum(
                jnp.sum(a.astype(jnp.float32) * b, axis=0, keepdims=True)
                for a, b in zip(half, weight_grads)
            )
            score_grads = [
                (a * (b - row_dots)).astype(jnp.bfloat16) for a, b in zip(weights, weight_grads)
            ]
            finish(
                queries,
                scaling * (dot(score_grads[0], keys[0], TN) + dot(score_grads[1], keys[1], TN)),
            )
            own_k_ref[...] += dot(score_grads[0], queries, NN)
            own_v_ref[...] += dot(half[0], grads, NN)
            acc_k[other] += dot(score_grads[1], queries, NN)
            acc_v[other] += dot(half[1], grads, NN)

    own_k_ref[...] = own_k_ref[...] * scaling
    part_k_ref[...] = (acc_k[...] * scaling).astype(jnp.bfloat16)
    part_v_ref[...] = acc_v[...].astype(jnp.bfloat16)


def attend(q, g, bias, k, v, kall, vall, other, count):
    rows, width = q.shape
    blocks = kall.shape[0]
    heads = other.shape[0]
    head_dim = width // heads
    kv_count = k.shape[1] // head_dim
    group = heads // kv_count
    wide = pl.BlockSpec((rows, group * head_dim), lambda s, *_: (0, s))
    thin = pl.BlockSpec((rows, head_dim), lambda s, *_: (0, s))
    line = pl.BlockSpec((1, group * head_dim), lambda s, *_: (0, s))
    whole = pl.BlockSpec((blocks, rows, head_dim), lambda s, *_: (0, 0, s))
    return pl.pallas_call(
        functools.partial(attend_kernel, head_dim, group, head_dim ** (-0.5)),
        grid_spec=pltpu.PrefetchScalarGridSpec(
            num_scalar_prefetch=2,
            grid=(kv_count,),
            in_specs=[wide, wide, line, thin, thin, whole, whole],
            out_specs=[wide, whole, whole, thin, thin, line],
            scratch_shapes=[
                pltpu.VMEM((blocks, rows, head_dim), jnp.float32),
                pltpu.VMEM((blocks, rows, head_dim), jnp.float32),
            ],
        ),
        out_shape=[
            jax.ShapeDtypeStruct((rows, width), jnp.bfloat16),
            jax.ShapeDtypeStruct(kall.shape, jnp.bfloat16),
            jax.ShapeDtypeStruct(vall.shape, jnp.bfloat16),
            jax.ShapeDtypeStruct(k.shape, jnp.float32),
            jax.ShapeDtypeStruct(v.shape, jnp.float32),
            jax.ShapeDtypeStruct((1, width), jnp.float32),
        ],
        compiler_params=pltpu.CompilerParams(vmem_limit_bytes=56 * 1024 * 1024),
        name="attend",
    )(other, count, q, g, bias, k, v, kall, vall)


MESH = pl.DeviceIdType.MESH


def place():
    me = lax.axis_index("seq")
    n = lax.axis_size("seq")
    lines = n // 4
    z, p = me // 4, me % 4
    x, y = p % 2, p // 2
    px = y * 2 + (1 - x)
    py = (1 - y) * 2 + x
    far = (1 - y) * 2 + (1 - x)
    return lines, z, p, px, py, far


def greet(targets, extra=()):
    barrier = pltpu.get_barrier_semaphore()
    for target in targets:
        pl.semaphore_signal(barrier, inc=1, device_id={"seq": target}, device_id_type=MESH)
    for target in extra:
        pl.semaphore_signal(barrier, inc=1, device_id={"rep": target}, device_id_type=MESH)
    pl.semaphore_wait(barrier, len(targets) + len(extra))


class Sender:
    def __init__(self, send_sem, recv_sem):
        self.send_sem, self.recv_sem, self.next, self.open = send_sem, recv_sem, 0, []

    def __call__(self, src, dst, **target):
        copy = pltpu.make_async_remote_copy(
            src_ref=src,
            dst_ref=dst,
            send_sem=self.send_sem.at[self.next],
            recv_sem=self.recv_sem.at[self.next],
            device_id=target,
            device_id_type=MESH,
        )
        self.next += 1
        copy.start()
        self.open.append(copy)
        return copy

    def drain(self):
        for copy in self.open:
            copy.wait_send()


def gather_kernel(k_ref, v_ref, kall_ref, vall_ref, send_sem, recv_sem, local_sem):
    lines, z, p, px, py, far = place()
    me = z * 4 + p
    zs = [lax.rem(z + lines - d, lines) for d in range(lines)]
    up = [lax.rem(z + d, lines) for d in range(lines)]
    greet([up[d] * 4 + p for d in range(1, lines)] + [z * 4 + px, z * 4 + py])
    send = Sender(send_sem, recv_sem)
    arrays = [(k_ref, kall_ref, px, py), (v_ref, vall_ref, py, px)]
    along, first, last = {}, {}, []
    own = []
    for a, (src, out, f, s) in enumerate(arrays):
        own.append(pltpu.make_async_copy(src, out.at[me], local_sem.at[a]))
        own[-1].start()
    for d in range(1, lines):
        for a, (src, out, f, s) in enumerate(arrays):
            along[a, d] = send(src, out.at[me], seq=up[d] * 4 + p)
    for d in range(lines + 1):
        if d < lines:
            for a, (src, out, f, s) in enumerate(arrays):
                spot = zs[d] * 4 + p
                if d:
                    along[a, d].wait_recv()
                piece = out.at[spot] if d else src
                first[a, d] = send(piece, out.at[spot], seq=z * 4 + f)
            for a, (src, out, f, s) in enumerate(arrays):
                spot = zs[d] * 4 + p
                piece = out.at[spot] if d else src
                last.append(send(piece, out.at[spot], seq=z * 4 + s))
        if d:
            for a, (src, out, f, s) in enumerate(arrays):
                spot = zs[d - 1] * 4 + f
                first[a, d - 1].wait_recv()
                last.append(send(out.at[spot], out.at[spot], seq=z * 4 + s))
    for copy in last:
        copy.wait_recv()
    send.drain()
    for copy in own:
        copy.wait()


def gather(k, v):
    n = lax.axis_size("seq")
    assert n % 4 == 0
    copies = 2 * (n // 4 - 1 + 3 * (n // 4))
    spec = pl.BlockSpec(memory_space=pl.ANY)
    return pl.pallas_call(
        gather_kernel,
        in_specs=[spec, spec],
        out_specs=[spec, spec],
        out_shape=[jax.ShapeDtypeStruct((n,) + one.shape, one.dtype) for one in (k, v)],
        scratch_shapes=[
            pltpu.SemaphoreType.DMA((copies,)),
            pltpu.SemaphoreType.DMA((copies,)),
            pltpu.SemaphoreType.DMA((2,)),
        ],
        compiler_params=pltpu.CompilerParams(collective_id=1, has_side_effects=True),
        name="gather",
    )(k, v)


def scatter_kernel(
    part_k, part_v, own_k, own_v, bias_ref,
    dk_ref, dv_ref, dbq_ref,
    half_k, half_v, line_k, line_v, end_k, end_v,
    rep_slots, x_slots, y_slots, z_slots, sums, send_sem, recv_sem,
):
    lines, z, p, px, py, far = place()
    me = z * 4 + p
    reps, rep = lax.axis_size("rep"), lax.axis_index("rep")
    up = [lax.rem(z + d, lines) for d in range(lines)]
    others = [lax.rem(rep + d, reps) for d in range(1, reps)]
    greet([up[d] * 4 + p for d in range(1, lines)] + [z * 4 + px, z * 4 + py], others)
    send = Sender(send_sem, recv_sem)
    arrays = [
        (part_k, own_k, dk_ref, half_k, line_k, end_k, px, py),
        (part_v, own_v, dv_ref, half_v, line_v, end_v, py, px),
    ]
    order = list(range(1, lines)) + [0]

    rep_slots[rep] = bias_ref[...]
    bias = [send(bias_ref, rep_slots.at[rep], rep=other) for other in others]
    x, y = p % 2, p // 2
    near, cross, down, ends = {}, {}, {}, []
    for d in order:
        for a, (part, own, out, half, line, end, f, s) in enumerate(arrays):
            cross[a, d] = send(part.at[up[d] * 4 + far], half.at[d, 1], seq=z * 4 + s)
        for a, (part, own, out, half, line, end, f, s) in enumerate(arrays):
            near[a, d] = send(part.at[up[d] * 4 + s], half.at[d, 0], seq=z * 4 + s)

    def total(slots, count):
        result = slots[0]
        for j in range(1, count):
            result = result + slots[j]
        return result

    def relay(stage):
        nonlocal bias
        for copy in bias:
            copy.wait_recv()
        if stage == 0:
            sums[0] = total(rep_slots, reps)
            x_slots[x] = sums[0]
            bias = [send(sums.at[0], x_slots.at[x], seq=z * 4 + px)]
        elif stage == 1:
            sums[1] = total(x_slots, 2)
            y_slots[y] = sums[1]
            bias = [send(sums.at[1], y_slots.at[y], seq=z * 4 + py)]
        elif stage == 2:
            sums[2] = total(y_slots, 2)
            z_slots[z] = sums[2]
            bias = [
                send(sums.at[2], z_slots.at[z], seq=up[d] * 4 + p) for d in range(1, lines)
            ]
        else:
            dbq_ref[...] = total(z_slots, lines)

    stage = 0
    for j in range(lines + 1):
        if j < lines:
            d = order[j]
            for a, (part, own, out, half, line, end, f, s) in enumerate(arrays):
                cross[a, d].wait_recv()
                half[d, 1] = half[d, 1] + part[up[d] * 4 + f]
                down[a, d] = send(half.at[d, 1], line.at[d], seq=z * 4 + f)
            for a, (part, own, out, half, line, end, f, s) in enumerate(arrays):
                near[a, d].wait_recv()
        if stage < 3:
            relay(stage)
            stage += 1
        if j:
            d = order[j - 1]
            for a, (part, own, out, half, line, end, f, s) in enumerate(arrays):
                down[a, d].wait_recv()
                summed = (
                    half[d, 0].astype(jnp.float32)
                    + part[up[d] * 4 + p].astype(jnp.float32)
                    + line[d].astype(jnp.float32)
                )
                if d:
                    line[d] = summed.astype(jnp.bfloat16)
                    ends.append((a, d, send(line.at[d], end.at[d - 1], seq=up[d] * 4 + p)))
                else:
                    line[d] = summed.astype(jnp.bfloat16)
    while stage < 4:
        relay(stage)
        stage += 1
    for a, d, copy in ends:
        copy.wait_recv()
    for part, own, out, half, line, end, f, s in arrays:
        result = own[...] + line[0].astype(jnp.float32)
        for d in range(lines - 1):
            result = result + end[d].astype(jnp.float32)
        out[...] = result.astype(jnp.bfloat16)
    send.drain()


def scatter(part_k, part_v, own_k, own_v, bias):
    n, reps = lax.axis_size("seq"), lax.axis_size("rep")
    lines = n // 4
    block, kind = part_k.shape[1:], part_k.dtype
    copies = 2 * (4 * lines - 1) + (reps - 1) + 2 + (lines - 1)
    spec = pl.BlockSpec(memory_space=pltpu.VMEM)
    slots = [reps, 2, 2, lines, 3]
    return pl.pallas_call(
        scatter_kernel,
        in_specs=[spec] * 5,
        out_specs=[spec] * 3,
        out_shape=[
            jax.ShapeDtypeStruct(block, kind),
            jax.ShapeDtypeStruct(block, kind),
            jax.ShapeDtypeStruct(bias.shape, jnp.float32),
        ],
        scratch_shapes=[pltpu.VMEM((lines, 2) + block, kind)] * 2
        + [pltpu.VMEM((lines,) + block, kind)] * 2
        + [pltpu.VMEM((lines - 1,) + block, kind)] * 2
        + [pltpu.VMEM((count,) + bias.shape, jnp.float32) for count in slots]
        + [pltpu.SemaphoreType.DMA((copies,))] * 2,
        compiler_params=pltpu.CompilerParams(
            collective_id=2, has_side_effects=True, vmem_limit_bytes=60 * 1024 * 1024
        ),
        name="scatter",
    )(part_k, part_v, own_k, own_v, bias)


def body(q_lin, k_lin, value_projection, grad_out, q_bias, block_lists, block_counts):
    me = lax.axis_index("seq")
    assert block_lists.shape[1] == lax.axis_size("seq") and block_lists.shape[2] == 2
    lists = lax.dynamic_index_in_dim(block_lists, me, 1, keepdims=False)
    count = lax.dynamic_index_in_dim(block_counts, me, 1, keepdims=False)
    other = jnp.clip(lists[:, 1], 0, block_lists.shape[1] - 1)
    kall, vall = gather(k_lin[0], value_projection[0])
    dq, part_k, part_v, own_k, own_v, dbq = attend(
        q_lin[0], grad_out[0], q_bias[None], k_lin[0], value_projection[0], kall, vall, other, count
    )
    dk, dv, dbq = scatter(part_k, part_v, own_k, own_v, dbq.reshape(8, -1))
    return (dq[None], dk[None], dv[None], dbq.reshape(-1))


def solution(mesh):
    placed = (P("rep", "seq", None),) * 4 + (P(),) * 3
    return jax.shard_map(
        body,
        mesh=mesh,
        in_specs=placed,
        out_specs=(P("rep", "seq", None),) * 3 + (P(),),
        check_vma=False,
    )
```

```python
import functools

import jax
import jax.numpy as jnp
from jax import lax
from jax.experimental import pallas as pl
from jax.experimental.pallas import tpu as pltpu
from jax.sharding import PartitionSpec as P

NT = (((1,), (1,)), ((), ()))
TN = (((0,), (0,)), ((), ()))
NN = (((1,), (0,)), ((), ()))


def dot(a, b, dims):
    return lax.dot_general(a, b, dims, preferred_element_type=jnp.float32)


def attend_kernel(
    head_dim, group, scaling,
    other_ref, count_ref,
    q_ref, g_ref, bias_ref, k_ref, v_ref, kall_ref, vall_ref,
    dq_ref, part_k_ref, part_v_ref, own_k_ref, own_v_ref, dbq_ref,
    acc_k, acc_v,
):
    step = pl.program_id(0)
    acc_k[...] = jnp.zeros_like(acc_k)
    acc_v[...] = jnp.zeros_like(acc_v)

    def finish(columns, grad_q):
        dq_ref[:, columns] = grad_q.astype(jnp.bfloat16)
        dbq_ref[:, columns] = jnp.sum(grad_q, axis=0, keepdims=True)

    def rows(columns):
        queries = (q_ref[:, columns].astype(jnp.float32) + bias_ref[:, columns]).astype(
            jnp.bfloat16
        )
        return queries, g_ref[:, columns]

    own_k = own_v = None
    for member in range(group):
        columns = slice(member * head_dim, (member + 1) * head_dim)
        alone = jnp.where(count_ref[step * group + member] == 1, 1.0, 0.0)
        queries, grads = rows(columns)
        keys, values = k_ref[...], v_ref[...]
        scores = dot(keys, queries, NT) * scaling
        weights = jnp.exp(scores - jnp.max(scores, axis=0, keepdims=True))
        weights = weights * (alone / jnp.sum(weights, axis=0, keepdims=True))
        half = weights.astype(jnp.bfloat16)
        weight_grads = dot(values, grads, NT)
        row_dots = jnp.sum(half.astype(jnp.float32) * weight_grads, axis=0, keepdims=True)
        score_grads = (weights * (weight_grads - row_dots)).astype(jnp.bfloat16)
        finish(columns, scaling * dot(score_grads, keys, TN))
        more_k, more_v = dot(score_grads, queries, NN), dot(half, grads, NN)
        own_k = more_k if own_k is None else own_k + more_k
        own_v = more_v if own_v is None else own_v + more_v
    own_k_ref[...] = own_k
    own_v_ref[...] = own_v

    for member in range(group):
        head = step * group + member
        columns = slice(member * head_dim, (member + 1) * head_dim)
        count = count_ref[head]
        other = other_ref[head]

        @pl.when(count != 1)
        def _():
            queries, grads = rows(columns)
            keys = [k_ref[...], kall_ref[other]]
            values = [v_ref[...], vall_ref[other]]
            scores = [dot(one, queries, NT) * scaling for one in keys]
            top = jnp.maximum(
                jnp.max(scores[0], axis=0, keepdims=True), jnp.max(scores[1], axis=0, keepdims=True)
            )
            weights = [jnp.exp(one - top) for one in scores]
            total = jnp.sum(weights[0], axis=0, keepdims=True) + jnp.sum(
                weights[1], axis=0, keepdims=True
            )
            scale_to = 1.0 / total
            weights = [one * scale_to for one in weights]
            half = [one.astype(jnp.bfloat16) for one in weights]
            weight_grads = [dot(one, grads, NT) for one in values]
            row_dots = sum(
                jnp.sum(a.astype(jnp.float32) * b, axis=0, keepdims=True)
                for a, b in zip(half, weight_grads)
            )
            score_grads = [
                (a * (b - row_dots)).astype(jnp.bfloat16) for a, b in zip(weights, weight_grads)
            ]
            finish(
                columns,
                scaling * (dot(score_grads[0], keys[0], TN) + dot(score_grads[1], keys[1], TN)),
            )
            own_k_ref[...] += dot(score_grads[0], queries, NN)
            own_v_ref[...] += dot(half[0], grads, NN)
            acc_k[other] += dot(score_grads[1], queries, NN)
            acc_v[other] += dot(half[1], grads, NN)

    own_k_ref[...] = own_k_ref[...] * scaling
    part_k_ref[...] = (acc_k[...] * scaling).astype(jnp.bfloat16)
    part_v_ref[...] = acc_v[...].astype(jnp.bfloat16)


def attend(q, g, bias, k, v, kall, vall, other, count):
    rows, width = q.shape
    blocks = kall.shape[0]
    heads = other.shape[0]
    head_dim = width // heads
    kv_count = k.shape[1] // head_dim
    group = heads // kv_count
    wide = pl.BlockSpec((rows, group * head_dim), lambda s, *_: (0, s))
    thin = pl.BlockSpec((rows, head_dim), lambda s, *_: (0, s))
    line = pl.BlockSpec((1, group * head_dim), lambda s, *_: (0, s))
    whole = pl.BlockSpec((blocks, rows, head_dim), lambda s, *_: (0, 0, s))
    return pl.pallas_call(
        functools.partial(attend_kernel, head_dim, group, head_dim ** (-0.5)),
        grid_spec=pltpu.PrefetchScalarGridSpec(
            num_scalar_prefetch=2,
            grid=(kv_count,),
            in_specs=[wide, wide, line, thin, thin, whole, whole],
            out_specs=[wide, whole, whole, thin, thin, line],
            scratch_shapes=[
                pltpu.VMEM((blocks, rows, head_dim), jnp.float32),
                pltpu.VMEM((blocks, rows, head_dim), jnp.float32),
            ],
        ),
        out_shape=[
            jax.ShapeDtypeStruct((rows, width), jnp.bfloat16),
            jax.ShapeDtypeStruct(kall.shape, jnp.bfloat16),
            jax.ShapeDtypeStruct(vall.shape, jnp.bfloat16),
            jax.ShapeDtypeStruct(k.shape, jnp.float32),
            jax.ShapeDtypeStruct(v.shape, jnp.float32),
            jax.ShapeDtypeStruct((1, width), jnp.float32),
        ],
        compiler_params=pltpu.CompilerParams(vmem_limit_bytes=56 * 1024 * 1024),
        name="attend",
    )(other, count, q, g, bias, k, v, kall, vall)


MESH = pl.DeviceIdType.MESH


def place():
    me = lax.axis_index("seq")
    n = lax.axis_size("seq")
    lines = n // 4
    z, p = me // 4, me % 4
    x, y = p % 2, p // 2
    px = y * 2 + (1 - x)
    py = (1 - y) * 2 + x
    far = (1 - y) * 2 + (1 - x)
    return lines, z, p, px, py, far


def greet(targets, extra=()):
    barrier = pltpu.get_barrier_semaphore()
    for target in targets:
        pl.semaphore_signal(barrier, inc=1, device_id={"seq": target}, device_id_type=MESH)
    for target in extra:
        pl.semaphore_signal(barrier, inc=1, device_id={"rep": target}, device_id_type=MESH)
    pl.semaphore_wait(barrier, len(targets) + len(extra))


class Sender:
    def __init__(self, send_sem, recv_sem):
        self.send_sem, self.recv_sem, self.next, self.open = send_sem, recv_sem, 0, []

    def __call__(self, src, dst, **target):
        copy = pltpu.make_async_remote_copy(
            src_ref=src,
            dst_ref=dst,
            send_sem=self.send_sem.at[self.next],
            recv_sem=self.recv_sem.at[self.next],
            device_id=target,
            device_id_type=MESH,
        )
        self.next += 1
        copy.start()
        self.open.append(copy)
        return copy

    def drain(self):
        for copy in self.open:
            copy.wait_send()


def gather_kernel(k_ref, v_ref, kall_ref, vall_ref, send_sem, recv_sem, local_sem):
    lines, z, p, px, py, far = place()
    me = z * 4 + p
    zs = [lax.rem(z + lines - d, lines) for d in range(lines)]
    up = [lax.rem(z + d, lines) for d in range(lines)]
    greet([up[d] * 4 + p for d in range(1, lines)] + [z * 4 + px, z * 4 + py])
    send = Sender(send_sem, recv_sem)
    arrays = [(k_ref, kall_ref, px, py), (v_ref, vall_ref, py, px)]
    along, first, last = {}, {}, []
    own = []
    for a, (src, out, f, s) in enumerate(arrays):
        own.append(pltpu.make_async_copy(src, out.at[me], local_sem.at[a]))
        own[-1].start()
    for d in range(1, lines):
        for a, (src, out, f, s) in enumerate(arrays):
            along[a, d] = send(src, out.at[me], seq=up[d] * 4 + p)
    for d in range(lines + 1):
        if d < lines:
            for a, (src, out, f, s) in enumerate(arrays):
                spot = zs[d] * 4 + p
                if d:
                    along[a, d].wait_recv()
                piece = out.at[spot] if d else src
                first[a, d] = send(piece, out.at[spot], seq=z * 4 + f)
            for a, (src, out, f, s) in enumerate(arrays):
                spot = zs[d] * 4 + p
                piece = out.at[spot] if d else src
                last.append(send(piece, out.at[spot], seq=z * 4 + s))
        if d:
            for a, (src, out, f, s) in enumerate(arrays):
                spot = zs[d - 1] * 4 + f
                first[a, d - 1].wait_recv()
                last.append(send(out.at[spot], out.at[spot], seq=z * 4 + s))
    for copy in last:
        copy.wait_recv()
    send.drain()
    for copy in own:
        copy.wait()


def gather(k, v):
    n = lax.axis_size("seq")
    assert n % 4 == 0
    copies = 2 * (n // 4 - 1 + 3 * (n // 4))
    spec = pl.BlockSpec(memory_space=pl.ANY)
    return pl.pallas_call(
        gather_kernel,
        in_specs=[spec, spec],
        out_specs=[spec, spec],
        out_shape=[jax.ShapeDtypeStruct((n,) + one.shape, one.dtype) for one in (k, v)],
        scratch_shapes=[
            pltpu.SemaphoreType.DMA((copies,)),
            pltpu.SemaphoreType.DMA((copies,)),
            pltpu.SemaphoreType.DMA((2,)),
        ],
        compiler_params=pltpu.CompilerParams(collective_id=1, has_side_effects=True),
        name="gather",
    )(k, v)


def scatter_kernel(
    part_k, part_v, own_k, own_v, bias_ref,
    dk_ref, dv_ref, dbq_ref,
    half_k, half_v, line_k, line_v, end_k, end_v,
    rep_slots, x_slots, y_slots, z_slots, sums, send_sem, recv_sem,
):
    lines, z, p, px, py, far = place()
    me = z * 4 + p
    reps, rep = lax.axis_size("rep"), lax.axis_index("rep")
    up = [lax.rem(z + d, lines) for d in range(lines)]
    others = [lax.rem(rep + d, reps) for d in range(1, reps)]
    greet([up[d] * 4 + p for d in range(1, lines)] + [z * 4 + px, z * 4 + py], others)
    send = Sender(send_sem, recv_sem)
    arrays = [
        (part_k, own_k, dk_ref, half_k, line_k, end_k, px, py),
        (part_v, own_v, dv_ref, half_v, line_v, end_v, py, px),
    ]
    order = list(range(1, lines)) + [0]

    rep_slots[rep] = bias_ref[...]
    bias = [send(bias_ref, rep_slots.at[rep], rep=other) for other in others]
    x, y = p % 2, p // 2
    near, cross, down, ends = {}, {}, {}, []

    def open_step(j):
        if j >= lines:
            return
        d = order[j]
        for a, (part, own, out, half, line, end, f, s) in enumerate(arrays):
            cross[a, d] = send(part.at[up[d] * 4 + far], half.at[d, 1], seq=z * 4 + s)
        for a, (part, own, out, half, line, end, f, s) in enumerate(arrays):
            near[a, d] = send(part.at[up[d] * 4 + s], half.at[d, 0], seq=z * 4 + s)

    open_step(0)

    def total(slots, count):
        result = slots[0]
        for j in range(1, count):
            result = result + slots[j]
        return result

    def relay(stage):
        nonlocal bias
        for copy in bias:
            copy.wait_recv()
        if stage == 0:
            sums[0] = total(rep_slots, reps)
            x_slots[x] = sums[0]
            bias = [send(sums.at[0], x_slots.at[x], seq=z * 4 + px)]
        elif stage == 1:
            sums[1] = total(x_slots, 2)
            y_slots[y] = sums[1]
            bias = [send(sums.at[1], y_slots.at[y], seq=z * 4 + py)]
        elif stage == 2:
            sums[2] = total(y_slots, 2)
            z_slots[z] = sums[2]
            bias = [
                send(sums.at[2], z_slots.at[z], seq=up[d] * 4 + p) for d in range(1, lines)
            ]
        else:
            dbq_ref[...] = total(z_slots, lines)

    stage = 0
    for j in range(lines + 1):
        if j < lines:
            open_step(j + 1)
            d = order[j]
            for a, (part, own, out, half, line, end, f, s) in enumerate(arrays):
                cross[a, d].wait_recv()
                half[d, 1] = half[d, 1] + part[up[d] * 4 + f]
                down[a, d] = send(half.at[d, 1], line.at[d], seq=z * 4 + f)
            for a, (part, own, out, half, line, end, f, s) in enumerate(arrays):
                near[a, d].wait_recv()
        if stage < 3:
            relay(stage)
            stage += 1
        if j:
            d = order[j - 1]
            for a, (part, own, out, half, line, end, f, s) in enumerate(arrays):
                down[a, d].wait_recv()
                summed = (
                    half[d, 0].astype(jnp.float32)
                    + part[up[d] * 4 + p].astype(jnp.float32)
                    + line[d].astype(jnp.float32)
                )
                if d:
                    line[d] = summed.astype(jnp.bfloat16)
                    ends.append((a, d, send(line.at[d], end.at[d - 1], seq=up[d] * 4 + p)))
                else:
                    line[d] = summed.astype(jnp.bfloat16)
    while stage < 4:
        relay(stage)
        stage += 1
    for a, d, copy in ends:
        copy.wait_recv()
    for part, own, out, half, line, end, f, s in arrays:
        result = own[...] + line[0].astype(jnp.float32)
        for d in range(lines - 1):
            result = result + end[d].astype(jnp.float32)
        out[...] = result.astype(jnp.bfloat16)
    send.drain()


def scatter(part_k, part_v, own_k, own_v, bias):
    n, reps = lax.axis_size("seq"), lax.axis_size("rep")
    lines = n // 4
    block, kind = part_k.shape[1:], part_k.dtype
    copies = 2 * (4 * lines - 1) + (reps - 1) + 2 + (lines - 1)
    spec = pl.BlockSpec(memory_space=pltpu.VMEM)
    slots = [reps, 2, 2, lines, 3]
    return pl.pallas_call(
        scatter_kernel,
        in_specs=[spec] * 5,
        out_specs=[spec] * 3,
        out_shape=[
            jax.ShapeDtypeStruct(block, kind),
            jax.ShapeDtypeStruct(block, kind),
            jax.ShapeDtypeStruct(bias.shape, jnp.float32),
        ],
        scratch_shapes=[pltpu.VMEM((lines, 2) + block, kind)] * 2
        + [pltpu.VMEM((lines,) + block, kind)] * 2
        + [pltpu.VMEM((lines - 1,) + block, kind)] * 2
        + [pltpu.VMEM((count,) + bias.shape, jnp.float32) for count in slots]
        + [pltpu.SemaphoreType.DMA((copies,))] * 2,
        compiler_params=pltpu.CompilerParams(
            collective_id=2, has_side_effects=True, vmem_limit_bytes=60 * 1024 * 1024
        ),
        name="scatter",
    )(part_k, part_v, own_k, own_v, bias)


def body(q_lin, k_lin, value_projection, grad_out, q_bias, block_lists, block_counts):
    me = lax.axis_index("seq")
    assert block_lists.shape[1] == lax.axis_size("seq") and block_lists.shape[2] == 2
    lists = lax.dynamic_index_in_dim(block_lists, me, 1, keepdims=False)
    count = lax.dynamic_index_in_dim(block_counts, me, 1, keepdims=False)
    other = jnp.clip(lists[:, 1], 0, block_lists.shape[1] - 1)
    kall, vall = gather(k_lin[0], value_projection[0])
    dq, part_k, part_v, own_k, own_v, dbq = attend(
        q_lin[0], grad_out[0], q_bias[None], k_lin[0], value_projection[0], kall, vall, other, count
    )
    dk, dv, dbq = scatter(part_k, part_v, own_k, own_v, dbq)
    return (dq[None], dk[None], dv[None], dbq.reshape(-1))


def solution(mesh):
    placed = (P("rep", "seq", None),) * 4 + (P(),) * 3
    return jax.shard_map(
        body,
        mesh=mesh,
        in_specs=placed,
        out_specs=(P("rep", "seq", None),) * 3 + (P(),),
        check_vma=False,
    )
```

```python
import functools

import jax
import jax.numpy as jnp
from jax import lax
from jax.experimental import pallas as pl
from jax.experimental.pallas import tpu as pltpu
from jax.sharding import PartitionSpec as P

NT = (((1,), (1,)), ((), ()))
TN = (((0,), (0,)), ((), ()))
NN = (((1,), (0,)), ((), ()))


def dot(a, b, dims):
    return lax.dot_general(a, b, dims, preferred_element_type=jnp.float32)


def attend_kernel(
    head_dim, group, scaling,
    other_ref, count_ref,
    q_ref, g_ref, bias_ref, k_ref, v_ref, kall_ref, vall_ref,
    dq_ref, part_k_ref, part_v_ref, own_k_ref, own_v_ref, dbq_ref,
    acc_k, acc_v,
):
    step = pl.program_id(0)
    acc_k[...] = jnp.zeros_like(acc_k)
    acc_v[...] = jnp.zeros_like(acc_v)

    def finish(columns, grad_q):
        dq_ref[:, columns] = grad_q.astype(jnp.bfloat16)
        dbq_ref[:, columns] = jnp.sum(grad_q, axis=0, keepdims=True)

    def rows(columns):
        queries = (q_ref[:, columns].astype(jnp.float32) + bias_ref[:, columns]).astype(
            jnp.bfloat16
        )
        return queries, g_ref[:, columns]

    own_k = own_v = None
    for member in range(group):
        columns = slice(member * head_dim, (member + 1) * head_dim)
        alone = jnp.where(count_ref[step * group + member] == 1, 1.0, 0.0)
        queries, grads = rows(columns)
        keys, values = k_ref[...], v_ref[...]
        scores = dot(keys, queries, NT) * scaling
        weights = jnp.exp(scores - jnp.max(scores, axis=0, keepdims=True))
        weights = weights * (alone / jnp.sum(weights, axis=0, keepdims=True))
        half = weights.astype(jnp.bfloat16)
        weight_grads = dot(values, grads, NT)
        row_dots = jnp.sum(half.astype(jnp.float32) * weight_grads, axis=0, keepdims=True)
        score_grads = (weights * (weight_grads - row_dots)).astype(jnp.bfloat16)
        finish(columns, scaling * dot(score_grads, keys, TN))
        more_k, more_v = dot(score_grads, queries, NN), dot(half, grads, NN)
        own_k = more_k if own_k is None else own_k + more_k
        own_v = more_v if own_v is None else own_v + more_v
    own_k_ref[...] = own_k
    own_v_ref[...] = own_v

    for member in range(group):
        head = step * group + member
        columns = slice(member * head_dim, (member + 1) * head_dim)
        count = count_ref[head]
        other = other_ref[head]

        @pl.when(count != 1)
        def _():
            queries, grads = rows(columns)
            keys = [k_ref[...], kall_ref[other]]
            values = [v_ref[...], vall_ref[other]]
            scores = [dot(one, queries, NT) * scaling for one in keys]
            top = jnp.maximum(
                jnp.max(scores[0], axis=0, keepdims=True), jnp.max(scores[1], axis=0, keepdims=True)
            )
            weights = [jnp.exp(one - top) for one in scores]
            total = jnp.sum(weights[0], axis=0, keepdims=True) + jnp.sum(
                weights[1], axis=0, keepdims=True
            )
            scale_to = 1.0 / total
            weights = [one * scale_to for one in weights]
            half = [one.astype(jnp.bfloat16) for one in weights]
            weight_grads = [dot(one, grads, NT) for one in values]
            row_dots = sum(
                jnp.sum(a.astype(jnp.float32) * b, axis=0, keepdims=True)
                for a, b in zip(half, weight_grads)
            )
            score_grads = [
                (a * (b - row_dots)).astype(jnp.bfloat16) for a, b in zip(weights, weight_grads)
            ]
            finish(
                columns,
                scaling * (dot(score_grads[0], keys[0], TN) + dot(score_grads[1], keys[1], TN)),
            )
            own_k_ref[...] += dot(score_grads[0], queries, NN)
            own_v_ref[...] += dot(half[0], grads, NN)
            acc_k[other] += dot(score_grads[1], queries, NN)
            acc_v[other] += dot(half[1], grads, NN)

    own_k_ref[...] = own_k_ref[...] * scaling
    part_k_ref[...] = (acc_k[...] * scaling).astype(jnp.bfloat16)
    part_v_ref[...] = acc_v[...].astype(jnp.bfloat16)


def attend(q, g, bias, k, v, kall, vall, other, count):
    rows, width = q.shape
    blocks = kall.shape[0]
    heads = other.shape[0]
    head_dim = width // heads
    kv_count = k.shape[1] // head_dim
    group = heads // kv_count
    wide = pl.BlockSpec((rows, group * head_dim), lambda s, *_: (0, s))
    thin = pl.BlockSpec((rows, head_dim), lambda s, *_: (0, s))
    line = pl.BlockSpec((1, group * head_dim), lambda s, *_: (0, s))
    whole = pl.BlockSpec((blocks, rows, head_dim), lambda s, *_: (0, 0, s))
    return pl.pallas_call(
        functools.partial(attend_kernel, head_dim, group, head_dim ** (-0.5)),
        grid_spec=pltpu.PrefetchScalarGridSpec(
            num_scalar_prefetch=2,
            grid=(kv_count,),
            in_specs=[wide, wide, line, thin, thin, whole, whole],
            out_specs=[wide, whole, whole, thin, thin, line],
            scratch_shapes=[
                pltpu.VMEM((blocks, rows, head_dim), jnp.float32),
                pltpu.VMEM((blocks, rows, head_dim), jnp.float32),
            ],
        ),
        out_shape=[
            jax.ShapeDtypeStruct((rows, width), jnp.bfloat16),
            jax.ShapeDtypeStruct(kall.shape, jnp.bfloat16),
            jax.ShapeDtypeStruct(vall.shape, jnp.bfloat16),
            jax.ShapeDtypeStruct(k.shape, jnp.float32),
            jax.ShapeDtypeStruct(v.shape, jnp.float32),
            jax.ShapeDtypeStruct((1, width), jnp.float32),
        ],
        compiler_params=pltpu.CompilerParams(vmem_limit_bytes=56 * 1024 * 1024),
        name="attend",
    )(other, count, q, g, bias, k, v, kall, vall)


MESH = pl.DeviceIdType.MESH


def place():
    me = lax.axis_index("seq")
    n = lax.axis_size("seq")
    lines = n // 4
    z, p = me // 4, me % 4
    x, y = p % 2, p // 2
    px = y * 2 + (1 - x)
    py = (1 - y) * 2 + x
    far = (1 - y) * 2 + (1 - x)
    return lines, z, p, px, py, far


def greet(targets, extra=()):
    barrier = pltpu.get_barrier_semaphore()
    for target in targets:
        pl.semaphore_signal(barrier, inc=1, device_id={"seq": target}, device_id_type=MESH)
    for target in extra:
        pl.semaphore_signal(barrier, inc=1, device_id={"rep": target}, device_id_type=MESH)
    pl.semaphore_wait(barrier, len(targets) + len(extra))


class Sender:
    def __init__(self, send_sem, recv_sem):
        self.send_sem, self.recv_sem, self.next, self.open = send_sem, recv_sem, 0, []

    def __call__(self, src, dst, **target):
        copy = pltpu.make_async_remote_copy(
            src_ref=src,
            dst_ref=dst,
            send_sem=self.send_sem.at[self.next],
            recv_sem=self.recv_sem.at[self.next],
            device_id=target,
            device_id_type=MESH,
        )
        self.next += 1
        copy.start()
        self.open.append(copy)
        return copy

    def drain(self):
        for copy in self.open:
            copy.wait_send()


def gather_kernel(k_ref, v_ref, kall_ref, vall_ref, send_sem, recv_sem, local_sem):
    lines, z, p, px, py, far = place()
    me = z * 4 + p
    zs = [lax.rem(z + lines - d, lines) for d in range(lines)]
    up = [lax.rem(z + d, lines) for d in range(lines)]
    greet([up[d] * 4 + p for d in range(1, lines)] + [z * 4 + px, z * 4 + py])
    send = Sender(send_sem, recv_sem)
    arrays = [(k_ref, kall_ref, px, py), (v_ref, vall_ref, py, px)]
    along, first, last = {}, {}, []
    own = []
    for a, (src, out, f, s) in enumerate(arrays):
        own.append(pltpu.make_async_copy(src, out.at[me], local_sem.at[a]))
        own[-1].start()
    for d in range(1, lines):
        for a, (src, out, f, s) in enumerate(arrays):
            along[a, d] = send(src, out.at[me], seq=up[d] * 4 + p)
    for d in range(lines + 1):
        if d < lines:
            for a, (src, out, f, s) in enumerate(arrays):
                spot = zs[d] * 4 + p
                if d:
                    along[a, d].wait_recv()
                piece = out.at[spot] if d else src
                first[a, d] = send(piece, out.at[spot], seq=z * 4 + f)
            for a, (src, out, f, s) in enumerate(arrays):
                spot = zs[d] * 4 + p
                piece = out.at[spot] if d else src
                last.append(send(piece, out.at[spot], seq=z * 4 + s))
        if d:
            for a, (src, out, f, s) in enumerate(arrays):
                spot = zs[d - 1] * 4 + f
                first[a, d - 1].wait_recv()
                last.append(send(out.at[spot], out.at[spot], seq=z * 4 + s))
    for copy in last:
        copy.wait_recv()
    send.drain()
    for copy in own:
        copy.wait()


def gather(k, v):
    n = lax.axis_size("seq")
    assert n % 4 == 0
    copies = 2 * (n // 4 - 1 + 3 * (n // 4))
    spec = pl.BlockSpec(memory_space=pl.ANY)
    return pl.pallas_call(
        gather_kernel,
        in_specs=[spec, spec],
        out_specs=[spec, spec],
        out_shape=[jax.ShapeDtypeStruct((n,) + one.shape, one.dtype) for one in (k, v)],
        scratch_shapes=[
            pltpu.SemaphoreType.DMA((copies,)),
            pltpu.SemaphoreType.DMA((copies,)),
            pltpu.SemaphoreType.DMA((2,)),
        ],
        compiler_params=pltpu.CompilerParams(collective_id=1, has_side_effects=True),
        name="gather",
    )(k, v)


def scatter_kernel(
    part_k, part_v, own_k, own_v, bias_ref,
    dk_ref, dv_ref, dbq_ref,
    half_k, half_v, line_k, line_v, end_k, end_v,
    rep_slots, x_slots, y_slots, z_slots, sums, send_sem, recv_sem,
):
    lines, z, p, px, py, far = place()
    me = z * 4 + p
    reps, rep = lax.axis_size("rep"), lax.axis_index("rep")
    up = [lax.rem(z + d, lines) for d in range(lines)]
    others = [lax.rem(rep + d, reps) for d in range(1, reps)]
    greet([up[d] * 4 + p for d in range(1, lines)] + [z * 4 + px, z * 4 + py], others)
    send = Sender(send_sem, recv_sem)
    arrays = [
        (part_k, own_k, dk_ref, half_k, line_k, end_k, px, py),
        (part_v, own_v, dv_ref, half_v, line_v, end_v, py, px),
    ]
    order = list(range(1, lines)) + [0]

    rep_slots[rep] = bias_ref[...]
    bias = [send(bias_ref, rep_slots.at[rep], rep=other) for other in others]
    x, y = p % 2, p // 2
    near, cross, down, ends = {}, {}, {}, []

    def open_step(j):
        if j >= lines:
            return
        d = order[j]
        for a, (part, own, out, half, line, end, f, s) in enumerate(arrays):
            cross[a, d] = send(part.at[up[d] * 4 + far], half.at[d, 1], seq=z * 4 + s)
        for a, (part, own, out, half, line, end, f, s) in enumerate(arrays):
            near[a, d] = send(part.at[up[d] * 4 + s], half.at[d, 0], seq=z * 4 + s)

    open_step(0)
    open_step(1)

    def total(slots, count):
        result = slots[0]
        for j in range(1, count):
            result = result + slots[j]
        return result

    def relay(stage):
        nonlocal bias
        for copy in bias:
            copy.wait_recv()
        if stage == 0:
            sums[0] = total(rep_slots, reps)
            x_slots[x] = sums[0]
            bias = [send(sums.at[0], x_slots.at[x], seq=z * 4 + px)]
        elif stage == 1:
            sums[1] = total(x_slots, 2)
            y_slots[y] = sums[1]
            bias = [send(sums.at[1], y_slots.at[y], seq=z * 4 + py)]
        elif stage == 2:
            sums[2] = total(y_slots, 2)
            z_slots[z] = sums[2]
            bias = [
                send(sums.at[2], z_slots.at[z], seq=up[d] * 4 + p) for d in range(1, lines)
            ]
        else:
            dbq_ref[...] = total(z_slots, lines)

    stage = 0
    for j in range(lines + 1):
        if j < lines:
            d = order[j]
            for a, (part, own, out, half, line, end, f, s) in enumerate(arrays):
                cross[a, d].wait_recv()
                half[d, 1] = half[d, 1] + part[up[d] * 4 + f]
                down[a, d] = send(half.at[d, 1], line.at[d], seq=z * 4 + f)
            open_step(j + 2)
            for a, (part, own, out, half, line, end, f, s) in enumerate(arrays):
                near[a, d].wait_recv()
        if stage < 3:
            relay(stage)
            stage += 1
        if j:
            d = order[j - 1]
            for a, (part, own, out, half, line, end, f, s) in enumerate(arrays):
                down[a, d].wait_recv()
                summed = (
                    half[d, 0].astype(jnp.float32)
                    + part[up[d] * 4 + p].astype(jnp.float32)
                    + line[d].astype(jnp.float32)
                )
                if d:
                    line[d] = summed.astype(jnp.bfloat16)
                    ends.append((a, d, send(line.at[d], end.at[d - 1], seq=up[d] * 4 + p)))
                else:
                    line[d] = summed.astype(jnp.bfloat16)
    while stage < 4:
        relay(stage)
        stage += 1
    for a, d, copy in ends:
        copy.wait_recv()
    for part, own, out, half, line, end, f, s in arrays:
        result = own[...] + line[0].astype(jnp.float32)
        for d in range(lines - 1):
            result = result + end[d].astype(jnp.float32)
        out[...] = result.astype(jnp.bfloat16)
    send.drain()


def scatter(part_k, part_v, own_k, own_v, bias):
    n, reps = lax.axis_size("seq"), lax.axis_size("rep")
    lines = n // 4
    block, kind = part_k.shape[1:], part_k.dtype
    copies = 2 * (4 * lines - 1) + (reps - 1) + 2 + (lines - 1)
    spec = pl.BlockSpec(memory_space=pltpu.VMEM)
    slots = [reps, 2, 2, lines, 3]
    return pl.pallas_call(
        scatter_kernel,
        in_specs=[spec] * 5,
        out_specs=[spec] * 3,
        out_shape=[
            jax.ShapeDtypeStruct(block, kind),
            jax.ShapeDtypeStruct(block, kind),
            jax.ShapeDtypeStruct(bias.shape, jnp.float32),
        ],
        scratch_shapes=[pltpu.VMEM((lines, 2) + block, kind)] * 2
        + [pltpu.VMEM((lines,) + block, kind)] * 2
        + [pltpu.VMEM((lines - 1,) + block, kind)] * 2
        + [pltpu.VMEM((count,) + bias.shape, jnp.float32) for count in slots]
        + [pltpu.SemaphoreType.DMA((copies,))] * 2,
        compiler_params=pltpu.CompilerParams(
            collective_id=2, has_side_effects=True, vmem_limit_bytes=60 * 1024 * 1024
        ),
        name="scatter",
    )(part_k, part_v, own_k, own_v, bias)


def body(q_lin, k_lin, value_projection, grad_out, q_bias, block_lists, block_counts):
    me = lax.axis_index("seq")
    assert block_lists.shape[1] == lax.axis_size("seq") and block_lists.shape[2] == 2
    lists = lax.dynamic_index_in_dim(block_lists, me, 1, keepdims=False)
    count = lax.dynamic_index_in_dim(block_counts, me, 1, keepdims=False)
    other = jnp.clip(lists[:, 1], 0, block_lists.shape[1] - 1)
    kall, vall = gather(k_lin[0], value_projection[0])
    dq, part_k, part_v, own_k, own_v, dbq = attend(
        q_lin[0], grad_out[0], q_bias[None], k_lin[0], value_projection[0], kall, vall, other, count
    )
    dk, dv, dbq = scatter(part_k, part_v, own_k, own_v, dbq)
    return (dq[None], dk[None], dv[None], dbq.reshape(-1))


def solution(mesh):
    placed = (P("rep", "seq", None),) * 4 + (P(),) * 3
    return jax.shard_map(
        body,
        mesh=mesh,
        in_specs=placed,
        out_specs=(P("rep", "seq", None),) * 3 + (P(),),
        check_vma=False,
    )
```
